512 devices in a mesh: groups: 2 (over y), ep: 128 (over z, x), hp: 2 (over core).
Axes of the slice: x: 8, y: 2, z: 16, core: 2. Of those that a mesh axis runs over, the one named last changes fastest.
The devices are a block of a 8x8x16 slice.
Arguments:
- x_pre: bfloat16 [14336, 1536], P(('groups', 'ep')), parts along dimension 0, may hold values from -6 to 6
- x_dec: bfloat16 [2048, 1536], P(('groups', 'ep')), parts along dimension 0, may hold values from -6 to 6
- prefill_query_rows: bfloat16 [14336, 2048], P(('groups', 'ep'), 'hp'), parts along dimension 0, may hold values from -240 to 240
- prefill_key_values: bfloat16 [2, 14336, 256], P(None, ('groups', 'ep'), 'hp'), parts along dimension 1, may hold values from -6.1 to 6.1
- decode_query_rows: bfloat16 [2048, 2048], P(('groups', 'ep'), 'hp'), parts along dimension 0, may hold values from -240 to 240
- decode_key_values: bfloat16 [2, 2048, 256], P(None, ('groups', 'ep'), 'hp'), parts along dimension 1, may hold values from -6 to 6
- cache: bfloat16 [2, 2048, 128, 256], P(None, ('groups', 'ep'), None, 'hp'), parts along dimension 1, may hold values from -6.1 to 6.1
- cache_len: int32 [2048], P(('groups', 'ep')), parts along dimension 0, may hold values from 2 to 128
- sinks: float32 [32], P('hp'), may hold values from -1 to 5
- o_weight: bfloat16 [2048, 1536], P('hp', 'ep'), may hold values from -0.125 to 0.125
- norm_gain: float32 [1536], replicated, may hold values from 0.5 to 1.5
- expert_ids: int32 [16384, 4], P(('groups', 'ep')), parts along dimension 0, may hold values from 0 to 63, all different within a row; in each aligned block of 64 rows (0 to 63, 64 to 127, ...) at most 6 rows name the same one
- route_logits: float32 [16384, 4], P(('groups', 'ep')), parts along dimension 0, may hold values from -6 to 6
- w_gate_up: bfloat16 [128, 2, 1536, 768], P('ep', None, None, 'hp'), may hold values from -0.15625 to 0.15625
- w_down: bfloat16 [128, 768, 1536], P('ep', 'hp'), may hold values from -0.15625 to 0.15625
Outputs:
- layer_out: bfloat16 [16384, 1536], P(('groups', 'ep', 'hp')), parts along dimension 0
The draws below stay inside these ranges and needn't reach their ends.
There are 2 independent parts, one for each index of `groups`. The reference program is written for one: setup_inputs(seed, part) draws one part's arguments, and reference() takes and returns one part's arrays. A program takes and returns all parts, laid end to end along the dimension named above; an argument that names none is the same for every part. Nothing has to cross between parts.
Inputs may be any that keep to these rules, and one draw needn't show every extreme that they name: `expert_ids`: each row names 4 different experts; among the rows of one index of ep no expert is named by more than 6 rows, and in every draw some expert is named by exactly 6 rows of some index.
All inputs are finite; a program needn't handle non-finite values.
Results may differ from the reference program's by a relative error of at most 0.0065.
Values may be sent and summed in bfloat16 or wider, within the bound.
A program may use at most 64 MiB of HBM per device.

```python
import math
import jax
import jax.numpy as jnp
import numpy as np
from jax import lax

D = 1536
QUERY_HEADS = 32
LOCAL_KV_HEADS = 4
HEAD_SIZE = 64
FF = 1536
TOPK = 4
PREFILL_LOCAL = 56
DEC_DEV = 8
CACHE_POSITIONS = 128
EXPERTS = 64
PREFILL_TOKENS = 7168
DECODE_COUNT = 1024
TOK_DEV = 64
TOKENS = 8192
SLOT = 6
N_EP = 128


def prefill_index_pairs(key):
    base_offset = jax.random.normal(jax.random.fold_in(key, 11), (2, PREFILL_TOKENS, LOCAL_KV_HEADS * HEAD_SIZE), jnp.float32)
    return jnp.clip(base_offset, -6.1, 6.1)


def draw_prefill_key_values(key, part):
    return prefill_index_pairs(key).astype(jnp.bfloat16)


def draw_prefill_query_rows(key, part):
    base_offset = jnp.clip(jax.random.normal(jax.random.fold_in(key, 13), (PREFILL_TOKENS, QUERY_HEADS * HEAD_SIZE), jnp.float32), -6.0, 6.0)
    return jnp.clip(base_offset, -240.0, 240.0).astype(jnp.bfloat16)


def draw_cache(key, part):
    base_offset = jnp.clip(jax.random.normal(jax.random.fold_in(key, 22), (2, DECODE_COUNT, CACHE_POSITIONS, LOCAL_KV_HEADS * HEAD_SIZE), jnp.float32), -6.0, 6.0)
    return base_offset.astype(jnp.bfloat16)


def draw_decode_query_rows(key, part):
    base_offset = jnp.clip(jax.random.normal(jax.random.fold_in(key, 23), (DECODE_COUNT, QUERY_HEADS * HEAD_SIZE), jnp.float32), -6.0, 6.0)
    return jnp.clip(base_offset, -240.0, 240.0).astype(jnp.bfloat16)


def plant(values, key, smallest, top_value):
    shape = values.shape
    index_at = [jax.random.randint(jax.random.fold_in(key, axis), (), 0, shape[axis]) for axis in range(len(shape))]
    values = values.at[tuple(index_at)].set(smallest)
    longest = shape.index(max(shape))
    index_at[longest] = (index_at[longest] + 1) % shape[longest]
    return values.at[tuple(index_at)].set(top_value)


def shard_levels(stream_key, dims, pieces, least, largest):
    factor_of, own = 1.0, jax.random.fold_in(stream_key, 6)
    for axis_at, parts in pieces:
        draws = jnp.exp(jax.random.uniform(jax.random.fold_in(own, axis_at), (parts,), jnp.float32, least / len(pieces), largest / len(pieces)))
        factor_of = factor_of * jnp.repeat(draws, dims[axis_at] // parts).reshape([-1 if axis == axis_at else 1 for axis in range(len(dims))])
    return factor_of


def shared_out(key, own, number, rows, number_of, top, limit, lean):
    ranking = jax.random.permutation(key, number_of)
    heavy_load, ordinary = portions_of(number_of, rows * top, limit, lean, True), portions_of(number_of, rows * top, limit, lean, False)
    places = jnp.arange(number_of)

    def named(sizes, offset_by):
        used = int((sizes > 0).sum())
        fixed = max(1, used // 4)
        shifted = fixed + (places - fixed + offset_by * (used - fixed)) % max(1, number_of - fixed)
        return jnp.zeros((number_of,), jnp.int32).at[ranking[jnp.where(places < fixed, places, shifted)]].set(jnp.asarray(sizes, jnp.int32))

    sizes = jnp.where(number % 4 == 0, named(heavy_load, number // 4), named(ordinary, number - number // 4 - 1))
    mixed = jax.random.permutation(jax.random.fold_in(own, 3), number_of)
    giver, receiver = mixed[0:number_of // 2 * 2:2], mixed[1:number_of // 2 * 2:2]
    room = jnp.minimum(sizes[giver] - 1, limit - sizes[receiver]) // 2
    room = jnp.where((giver == ranking[0]) | (receiver == ranking[0]) | (sizes[receiver] == 0), 0, jnp.maximum(room, 0))
    shifted = jax.random.randint(jax.random.fold_in(own, 4), (number_of // 2,), 0, 1 << 20) % (room + 1)
    sizes = sizes.at[giver].add(-shifted).at[receiver].add(shifted)
    items = jnp.searchsorted(jnp.cumsum(sizes), jnp.arange(rows * top), side="right").astype(jnp.int32)
    grid = items.reshape(top, rows).T
    grid = grid[jax.random.permutation(jax.random.fold_in(own, 1), rows)]
    offset_by = jax.random.randint(jax.random.fold_in(own, 2), (rows, 1), 0, top)
    return jnp.take_along_axis(grid, (jnp.arange(top)[None, :] + offset_by) % top, axis=1)


def portions_of(number_of, total, most, skew, full):
    weights = [(1 << 20) // math.isqrt(rank ** skew) + 1 for rank in range(1, number_of + 1)]
    largest = most if full else min(most, max(-(-total // number_of), total * weights[0] // sum(weights)))
    least = 1 if total - largest >= number_of - 1 else 0
    given, spare = [largest] + [least] * (number_of - 1), total - largest - least * (number_of - 1)
    while spare > 0:
        candidates = [i for i in range(1, number_of) if given[i] < largest] or [i for i in range(1, number_of) if given[i] < most]
        whole, budget = sum([weights[i] for i in candidates]), spare
        for i in candidates:
            extra = min(most - given[i], max(1, budget * weights[i] // whole), spare)
            given[i] = given[i] + extra
            spare = spare - extra
    return np.array(given)


def centred(stream_key, extent, deviation, limit, split=(), held_as=jnp.bfloat16):
    array = deviation * jax.random.normal(stream_key, extent, jnp.float32)
    if split:
        array = array * shard_levels(stream_key, extent, split, -0.22, 0.18)
    return jnp.clip(array, -limit, limit).astype(held_as)


def setup_inputs(seed: int = 0, part: int = 0) -> dict:
    streams_of = jax.random.split(jax.random.key(seed), 16)
    part_keys = jax.random.split(jax.random.fold_in(streams_of[15], part), 16)
    x_pre = centred(part_keys[0], (PREFILL_TOKENS, D), 1.0, 6.0, ((0, 128),))
    x_dec = centred(part_keys[1], (DECODE_COUNT, D), 1.0, 6.0, ((0, 128),))
    prefill_query_rows = draw_prefill_query_rows(jax.random.fold_in(jax.random.fold_in(streams_of[15], part), 71), part)
    prefill_key_values = draw_prefill_key_values(jax.random.fold_in(jax.random.fold_in(streams_of[15], part), 71), part)
    decode_query_rows = draw_decode_query_rows(jax.random.fold_in(jax.random.fold_in(streams_of[15], part), 71), part)
    decode_key_values = centred(part_keys[5], (2, DECODE_COUNT, LOCAL_KV_HEADS * HEAD_SIZE), 1.0, 6.0, ((1, 128), (2, 2)))
    cache = draw_cache(jax.random.fold_in(jax.random.fold_in(streams_of[15], part), 71), part)
    cache_len = plant(jax.random.randint(part_keys[7], (DECODE_COUNT,), 2, CACHE_POSITIONS + 1), jax.random.fold_in(part_keys[7], 1), 2, CACHE_POSITIONS).astype(jnp.int32)
    sinks = jnp.clip(-1.0 + 6.0 * jax.random.uniform(streams_of[8], (QUERY_HEADS,), jnp.float32) ** shard_levels(streams_of[8], (QUERY_HEADS,), ((0, 2),), -0.2, 0.2), -1.0, 5.0)
    o_weight = centred(streams_of[9], (QUERY_HEADS * HEAD_SIZE, D), (QUERY_HEADS * HEAD_SIZE) ** -0.5, 0.125, ((0, 2), (1, 128)))
    norm_gain = jnp.clip(1.0 + 0.1 * jax.random.normal(streams_of[10], (D,), jnp.float32), 0.5, 1.5)
    expert_ids_keys = jax.random.split(jax.random.fold_in(part_keys[11], 1), TOKENS // TOK_DEV)
    expert_ids_turns = jax.random.permutation(jax.random.fold_in(part_keys[11], 3), TOKENS // TOK_DEV)
    expert_ids = jax.vmap(lambda own, number: shared_out(jax.random.fold_in(part_keys[11], 2), own, number, TOK_DEV, EXPERTS, TOPK, SLOT, 2))(expert_ids_keys, expert_ids_turns).reshape((TOKENS, TOPK))
    route_logits = centred(part_keys[12], (TOKENS, TOPK), 1.5, 6.0, ((0, 128),), jnp.float32)
    w_gate_up = centred(streams_of[13], (2 * EXPERTS, 2, D, FF // 2), D ** -0.5, 0.15625, ((0, 128), (3, 2)))
    w_down = centred(streams_of[14], (2 * EXPERTS, FF // 2, D), FF ** -0.5, 0.15625, ((0, 128), (1, 2)))
    return {"x_pre": x_pre, "x_dec": x_dec, "prefill_query_rows": prefill_query_rows, "prefill_key_values": prefill_key_values, "decode_query_rows": decode_query_rows, "decode_key_values": decode_key_values, "cache": cache, "cache_len": cache_len, "sinks": sinks, "o_weight": o_weight, "norm_gain": norm_gain, "expert_ids": expert_ids, "route_logits": route_logits, "w_gate_up": w_gate_up, "w_down": w_down}


EPS = 1e-05

def softmax_probability(scores, sink_logit_bias):
    top = jnp.maximum(lax.optimization_barrier(jnp.max(scores, axis=-1, keepdims=True)), sink_logit_bias)
    expo = jnp.exp(scores - top)
    total = lax.optimization_barrier(jnp.sum(expo, axis=-1, keepdims=True)) + jnp.exp(sink_logit_bias - top)
    return (expo / total).astype(jnp.bfloat16)

def prefill_attention(prefill_query_rows, prefill_key_values, sinks):
    head_group = QUERY_HEADS // LOCAL_KV_HEADS
    block_list = PREFILL_TOKENS // PREFILL_LOCAL
    key_rows = prefill_key_values[0].reshape(block_list, PREFILL_LOCAL, LOCAL_KV_HEADS, HEAD_SIZE)
    value_rows = prefill_key_values[1].reshape(block_list, PREFILL_LOCAL, LOCAL_KV_HEADS, HEAD_SIZE)
    query_rows = prefill_query_rows.reshape(block_list, PREFILL_LOCAL, LOCAL_KV_HEADS, head_group, HEAD_SIZE)
    sink_logit_bias = sinks.reshape(LOCAL_KV_HEADS, head_group)[None, :, :, None]
    places = jnp.arange(PREFILL_LOCAL, dtype=jnp.int32)
    visible = places[None, :] <= places[:, None]

    def one_block(args):
        rows, block_keys, block_values = args
        scores = jnp.einsum('qhgd,khd->qhgk', rows.astype(jnp.float32), block_keys.astype(jnp.float32)) * HEAD_SIZE ** (-0.5)
        scores = jnp.where(visible[:, None, None, :], scores, -jnp.inf)
        weight_matrix = softmax_probability(scores, sink_logit_bias)
        out = jnp.einsum('qhgk,khd->qhgd', weight_matrix.astype(jnp.float32), block_values.astype(jnp.float32))
        return out.astype(jnp.bfloat16).reshape(PREFILL_LOCAL, QUERY_HEADS * HEAD_SIZE)
    return lax.map(one_block, (query_rows, key_rows, value_rows)).reshape(PREFILL_TOKENS, QUERY_HEADS * HEAD_SIZE)

def decode_attention(decode_query_rows, decode_key_values, cache, cache_len, sinks):
    head_group = QUERY_HEADS // LOCAL_KV_HEADS
    query_rows = decode_query_rows.reshape(DECODE_COUNT, LOCAL_KV_HEADS, head_group, HEAD_SIZE).astype(jnp.float32)
    cached_key_rows = cache[0].reshape(DECODE_COUNT, CACHE_POSITIONS, LOCAL_KV_HEADS, HEAD_SIZE).astype(jnp.float32)
    cached_value_rows = cache[1].reshape(DECODE_COUNT, CACHE_POSITIONS, LOCAL_KV_HEADS, HEAD_SIZE).astype(jnp.float32)
    own_key_rows = decode_key_values[0].reshape(DECODE_COUNT, LOCAL_KV_HEADS, HEAD_SIZE).astype(jnp.float32)
    own_value_rows = decode_key_values[1].reshape(DECODE_COUNT, LOCAL_KV_HEADS, HEAD_SIZE).astype(jnp.float32)
    past_positions = jnp.einsum('shgd,sjhd->shgj', query_rows, cached_key_rows) * HEAD_SIZE ** (-0.5)
    live = jnp.arange(CACHE_POSITIONS, dtype=jnp.int32)[None, :] < cache_len[:, None]
    past_positions = jnp.where(live[:, None, None, :], past_positions, -jnp.inf)
    own_token = jnp.einsum('shgd,shd->shg', query_rows, own_key_rows)[..., None] * HEAD_SIZE ** (-0.5)
    weight_matrix = softmax_probability(jnp.concatenate([past_positions, own_token], axis=-1), sinks.reshape(LOCAL_KV_HEADS, head_group)[None, :, :, None])
    weight_matrix = weight_matrix.astype(jnp.float32)
    out = jnp.einsum('shgj,sjhd->shgd', weight_matrix[..., :CACHE_POSITIONS], cached_value_rows)
    out = out + weight_matrix[..., CACHE_POSITIONS:] * own_value_rows[:, :, None, :]
    return out.astype(jnp.bfloat16).reshape(DECODE_COUNT, QUERY_HEADS * HEAD_SIZE)

def device_major(pre, dec):
    first = pre.reshape(N_EP, PREFILL_LOCAL, pre.shape[-1])
    second = dec.reshape(N_EP, DEC_DEV, dec.shape[-1])
    return jnp.concatenate([first, second], axis=1).reshape(N_EP * (PREFILL_LOCAL + DEC_DEV), pre.shape[-1])

def reference(x_pre, x_dec, prefill_query_rows, prefill_key_values, decode_query_rows, decode_key_values, cache, cache_len, sinks, o_weight, norm_gain, expert_ids, route_logits, w_gate_up, w_down):
    attended = device_major(prefill_attention(prefill_query_rows, prefill_key_values, sinks), decode_attention(decode_query_rows, decode_key_values, cache, cache_len, sinks))
    stream = device_major(x_pre, x_dec).astype(jnp.float32) + jnp.dot(attended, o_weight, preferred_element_type=jnp.float32)
    mean_sq = lax.optimization_barrier(jnp.mean(stream * stream, axis=-1, keepdims=True))
    normed = (stream * lax.rsqrt(mean_sq + EPS) * norm_gain).astype(jnp.bfloat16)
    flat_ids = expert_ids.reshape(-1)
    capacity = N_EP * SLOT
    quarter = FF // 4

    def one_holder(outputs, args):
        expert, gate_up, down = args
        chosen = flat_ids == expert
        picked = jnp.nonzero(chosen, size=capacity, fill_value=0)[0].astype(jnp.int32)
        count = jnp.sum(chosen.astype(jnp.int32))
        live = (jnp.arange(capacity, dtype=jnp.int32) < count).astype(jnp.float32)
        rows = normed[picked // TOPK]
        gate = jnp.dot(rows, gate_up[0], preferred_element_type=jnp.float32)
        upper = jnp.dot(rows, gate_up[1], preferred_element_type=jnp.float32)
        hidden = ((upper + 1.0) * gate * jax.nn.sigmoid(1.702 * gate)).astype(jnp.bfloat16)
        lower_part = jnp.dot(hidden[:, :quarter], down[:quarter], preferred_element_type=jnp.float32).astype(jnp.bfloat16)
        upper_part = jnp.dot(hidden[:, quarter:], down[quarter:], preferred_element_type=jnp.float32).astype(jnp.bfloat16)
        lower_part, upper_part = lax.optimization_barrier((lower_part, upper_part))
        result = (lower_part.astype(jnp.float32) + upper_part.astype(jnp.float32)).astype(jnp.bfloat16)
        result = lax.optimization_barrier(result).astype(jnp.float32) * live[:, None]
        return (outputs.at[picked].add(result), None)
    holders = jnp.arange(2 * EXPERTS, dtype=jnp.int32) // 2
    outputs, _ = lax.scan(one_holder, jnp.zeros((TOKENS * TOPK, D), jnp.float32), (holders, w_gate_up, w_down))
    mix = jax.nn.softmax(route_logits, axis=-1)
    moe = lax.optimization_barrier(jnp.sum(outputs.reshape(TOKENS, TOPK, D) * mix[:, :, None], axis=1))
    return (stream + moe).astype(jnp.bfloat16)
```

```python
import functools

import jax
import jax.numpy as jnp
import numpy as np
from jax import lax
from jax.experimental import pallas as pl
from jax.experimental.pallas import tpu as pltpu
from jax.sharding import Mesh
from jax.sharding import PartitionSpec as P

HEAD_SIZE = 64
EP = ("ep_0", "ep_1")
GROUPS_EP = ("groups", "ep_0", "ep_1")
GROUPS_EP_HP = ("groups", "ep_0", "ep_1", "hp")
EPS = 1e-05
MESH = pl.DeviceIdType.MESH
F32 = jnp.float32
BF16 = jnp.bfloat16


def softmax_probability(scores, sink_logit_bias):
    top = jnp.maximum(jnp.max(scores, axis=-1, keepdims=True), sink_logit_bias)
    expo = jnp.exp(scores - top)
    total = jnp.sum(expo, axis=-1, keepdims=True) + jnp.exp(sink_logit_bias - top)
    return (expo / total).astype(BF16)


def attention(
    prefill_query_rows,
    prefill_key_values,
    decode_query_rows,
    decode_key_values,
    cache,
    cache_len,
    sinks,
):
    pre_rows = prefill_query_rows.shape[0]
    dec_rows = decode_query_rows.shape[0]
    kv_heads = prefill_key_values.shape[2] // HEAD_SIZE
    q_heads = sinks.shape[0]
    head_group = q_heads // kv_heads
    kv_max = cache.shape[2]
    scale = HEAD_SIZE ** (-0.5)
    sink_logit_bias = sinks.reshape(kv_heads, head_group)[None, :, :, None]
    keys_here = prefill_key_values[0].reshape(pre_rows, kv_heads, HEAD_SIZE)
    values_here = prefill_key_values[1].reshape(pre_rows, kv_heads, HEAD_SIZE)
    query_rows = prefill_query_rows.reshape(pre_rows, kv_heads, head_group, HEAD_SIZE)
    scores = jnp.einsum("qhgd,khd->qhgk", query_rows, keys_here, preferred_element_type=F32) * scale
    places = jnp.arange(pre_rows, dtype=jnp.int32)
    visible = places[None, :] <= places[:, None]
    scores = jnp.where(visible[:, None, None, :], scores, -jnp.inf)
    weight_matrix = softmax_probability(scores, sink_logit_bias)
    pre_out = jnp.einsum("qhgk,khd->qhgd", weight_matrix, values_here, preferred_element_type=F32)
    pre_out = pre_out.astype(BF16).reshape(pre_rows, q_heads * HEAD_SIZE)
    dec_queries = decode_query_rows.reshape(dec_rows, kv_heads, head_group, HEAD_SIZE)
    cached_key_rows = cache[0].reshape(dec_rows, kv_max, kv_heads, HEAD_SIZE)
    cached_value_rows = cache[1].reshape(dec_rows, kv_max, kv_heads, HEAD_SIZE)
    own_key_rows = decode_key_values[0].reshape(dec_rows, kv_heads, HEAD_SIZE)
    own_value_rows = decode_key_values[1].reshape(dec_rows, kv_heads, HEAD_SIZE)
    past_positions = (
        jnp.einsum("shgd,sjhd->shgj", dec_queries, cached_key_rows, preferred_element_type=F32) * scale
    )
    live = jnp.arange(kv_max, dtype=jnp.int32)[None, :] < cache_len[:, None]
    past_positions = jnp.where(live[:, None, None, :], past_positions, -jnp.inf)
    own_token = (
        jnp.einsum("shgd,shd->shg", dec_queries, own_key_rows, preferred_element_type=F32)[..., None]
        * scale
    )
    dec_weights = softmax_probability(
        jnp.concatenate([past_positions, own_token], axis=-1), sink_logit_bias
    )
    dec_out = jnp.einsum(
        "shgj,sjhd->shgd", dec_weights[..., :kv_max], cached_value_rows, preferred_element_type=F32
    )
    dec_out = (
        dec_out
        + dec_weights[..., kv_max:].astype(F32) * own_value_rows.astype(F32)[:, :, None, :]
    )
    dec_out = dec_out.astype(BF16).reshape(dec_rows, q_heads * HEAD_SIZE)
    return jnp.concatenate([pre_out, dec_out], axis=0)


def remote(src, dst, send_sem, recv_sem, where):
    return pltpu.make_async_remote_copy(
        src_ref=src,
        dst_ref=dst,
        send_sem=send_sem,
        recv_sem=recv_sem,
        device_id=where,
        device_id_type=MESH,
    )


def greet(places):
    barrier = pltpu.get_barrier_semaphore()
    for place in places:
        pl.semaphore_signal(barrier, inc=1, device_id=place, device_id_type=MESH)
    pl.semaphore_wait(barrier, len(places))


def shifted(me, by, n):
    return lax.rem(me + (by + 2 * n), n)


def ring_gather(axis, n, me, view, subs, send_sems, recv_sems, sent):
    half = n // 2
    ways = ((0, -1, shifted(me, 1, n)), (1, 1, shifted(me, -1, n)))

    def used(step, way, sub):
        return step < half or sub % 2 == way

    def copy(step, way, sign, to, sub):
        block = view(shifted(me, sign * (step - 1), n), sub)
        at = (way * half + step - 1) * subs + sub
        return remote(block, block, send_sems.at[at], recv_sems.at[at], {axis: to})

    def arrival(step, way, sign, to, sub):
        block = view(shifted(me, sign * step, n), sub)
        at = (way * half + step - 1) * subs + sub
        return remote(block, block, send_sems.at[at], recv_sems.at[at], {axis: to})

    for sub in range(subs):
        for way, sign, to in ways:
            if used(1, way, sub):
                c = copy(1, way, sign, to, sub)
                c.start()
                sent.append(c)
    yield
    for step in range(1, half + 1):
        for sub in range(subs):
            for way, sign, to in ways:
                if not used(step, way, sub):
                    continue
                arrival(step, way, sign, to, sub).wait_recv()
                if step < half and used(step + 1, way, sub):
                    c = copy(step + 1, way, sign, to, sub)
                    c.start()
                    sent.append(c)
        yield


def ring_sems(n, subs):
    return pltpu.SemaphoreType.DMA((n * subs,))


def in_turn(*rings):
    rings = list(rings)
    while rings:
        for ring in list(rings):
            try:
                next(ring)
            except StopIteration:
                rings.remove(ring)


def nt(a, b):
    return lax.dot_general(a, b, (((1,), (1,)), ((), ())), preferred_element_type=F32)


def project_kernel(
    nz,
    nx,
    width_of,
    weight,
    attn,
    x_pre,
    x_dec,
    gain,
    info,
    pick_a,
    pick_b,
    stream,
    normed,
    info_all,
    small_a,
    small_b,
    big_a,
    big_b,
    sum_a,
    sum_b,
    from_core,
    squares,
    squares_in,
    small_a_send,
    small_a_recv,
    small_b_send,
    small_b_recv,
    big_a_send,
    big_a_recv,
    big_b_send,
    big_b_recv,
    info_send,
    info_recv,
    core_send,
    core_recv,
):
    z, x, h = lax.axis_index("ep_0"), lax.axis_index("ep_1"), lax.axis_index("hp")
    other = 1 - h
    greet(
        [
            {"ep_0": shifted(z, 1, nz)},
            {"ep_0": shifted(z, -1, nz)},
            {"ep_1": shifted(x, 1, nx)},
            {"ep_1": shifted(x, -1, nx)},
            {"hp": other},
        ]
    )
    k_half = weight.shape[1] // 2
    tokens = stream.shape[0]
    cols = stream.shape[1]
    small_a[x] = weight[:, 0:k_half]
    small_b[z] = weight[:, k_half : 2 * k_half]
    info_all[z] = info[...]
    sent = []
    ring_a = ring_gather(
        "ep_1", nx, x, lambda b, s: small_a.at[b], 1, small_a_send, small_a_recv, sent
    )
    ring_b = ring_gather(
        "ep_0", nz, z, lambda b, s: small_b.at[b], 1, small_b_send, small_b_recv, sent
    )
    next(ring_a)
    next(ring_b)
    for _ in range(nx // 2):
        next(ring_a)
    a_rows = big_a.shape[1]
    b_rows = big_b.shape[1]
    packed = jnp.dot(
        pick_a[...], small_a[...].reshape(-1, k_half), preferred_element_type=F32
    ).astype(BF16)
    big_a[z] = packed
    large_a = ring_gather(
        "ep_0",
        nz,
        z,
        lambda b, s: big_a.at[b, pl.ds(s * (a_rows // 2), a_rows // 2), :],
        2,
        big_a_send,
        big_a_recv,
        sent,
    )
    next(large_a)
    for _ in range(nz // 2):
        next(ring_b)
    packed = jnp.dot(
        pick_b[...], small_b[...].reshape(-1, k_half), preferred_element_type=F32
    ).astype(BF16)
    big_b[x] = packed
    large_b = ring_gather(
        "ep_1",
        nx,
        x,
        lambda b, s: big_b.at[b, pl.ds(s * (b_rows // 4), b_rows // 4), :],
        4,
        big_b_send,
        big_b_recv,
        sent,
    )
    next(large_b)
    tell = ring_gather("ep_0", nz, z, lambda b, s: info_all.at[b], 1, info_send, info_recv, sent)
    next(tell)
    for step in range(1, nz // 2 + 1):
        next(large_a)
        if step % (nz // nx) == 0:
            next(large_b)
        next(tell)
    attn_a = attn[:, 0:k_half]
    attn_b = attn[:, k_half : 2 * k_half]
    for b in range(nz):
        sum_a[b * a_rows : (b + 1) * a_rows, :] = nt(big_a[b], attn_a)
    for b in range(nx):
        sum_b[b * b_rows : (b + 1) * b_rows, :] = nt(big_b[b], attn_b)
    w = width_of
    for b in range(nz):
        for c in range(nx):
            at_a = (b * nx + c) * w
            at_b = (c * nz + b) * w
            sum_a[at_a : at_a + w, :] = sum_a[at_a : at_a + w, :] + sum_b[at_b : at_b + w, :]
    mine = pl.multiple_of(h * cols, cols)
    theirs = pl.multiple_of(other * cols, cols)
    swap = remote(
        sum_a.at[pl.ds(theirs, cols), :],
        from_core,
        core_send.at[0],
        core_recv.at[0],
        {"hp": other},
    )
    swap.start()
    swap.wait()
    summed = jnp.transpose(sum_a[pl.ds(mine, cols), :] + from_core[...])
    n_pre = x_pre.shape[0]
    stream[0:n_pre, :] = summed[0:n_pre] + x_pre[:, pl.ds(mine, cols)].astype(F32)
    stream[n_pre:tokens, :] = summed[n_pre:tokens] + x_dec[:, pl.ds(mine, cols)].astype(F32)
    value = stream[...]
    total = jnp.sum(value * value, axis=-1, keepdims=True)
    squares[...] = jnp.broadcast_to(total, squares.shape)
    swap = remote(squares, squares_in, core_send.at[1], core_recv.at[1], {"hp": other})
    swap.start()
    swap.wait()
    total = total + squares_in[:, 0:1]
    scale = lax.rsqrt(total / (2 * cols) + EPS)
    normed[...] = (value * scale * gain[:, pl.ds(mine, cols)]).astype(BF16)
    for c in sent:
        c.wait_send()


def places_around(nz, nx):
    z, x, h = lax.axis_index("ep_0"), lax.axis_index("ep_1"), lax.axis_index("hp")
    sign = 1 - 2 * lax.rem(x, 2)

    def near(by):
        return lax.rem(x + by * sign + 2 * nx, nx)

    return z, x, h, near


REACH = {1: -1, 2: 2, 3: -3}
ORDER = (3, 2, 1)


def friends(nz, z, h, near):
    return [
        {"ep_0": shifted(z, 1, nz)},
        {"ep_0": shifted(z, -1, nz)},
        {"hp": 1 - h},
        {"ep_1": near(1)},
        {"ep_1": near(-1)},
        {"ep_1": near(2)},
        {"ep_1": near(-2)},
        {"ep_1": near(-3)},
    ]


def dispatch_kernel(
    nz,
    nx,
    normed,
    info_all,
    rows,
    tok,
    onehot,
    picked,
    z_send,
    z_recv,
    direct_send,
    direct_recv,
    pair_send,
    pair_recv,
    core_send,
    core_recv,
):
    z, x, h, near = places_around(nz, nx)
    other = 1 - h
    greet(friends(nz, z, h, near))
    tokens, cols = normed.shape
    pairs, per_pair = picked.shape[0], picked.shape[1]
    tok[z] = normed[...]
    sent = []
    part = tokens // 2
    ring = ring_gather(
        "ep_0", nz, z, lambda b, s: tok.at[b, pl.ds(s * part, part), :], 2, z_send, z_recv, sent
    )
    next(ring)
    slots = pairs * per_pair
    first = (z * slots).astype(F32)
    target = lax.broadcasted_iota(jnp.int32, (slots, 128), 0).astype(F32) + first
    lower = lax.broadcasted_iota(jnp.int32, (8, 128), 1) < tokens
    for j in range(nz // 2):
        codes = jnp.where(lower, info_all[2 * j], info_all[2 * j + 1])
        hit = jnp.zeros((slots, 128), F32)
        for k in range(4):
            hit = jnp.where(codes[k : k + 1, :] == target, 1.0, hit)
        onehot[:, 128 * j : 128 * (j + 1)] = hit.astype(BF16)
    for _ in range(nz // 2):
        next(ring)
    everything = tok[...].reshape(nz * tokens, cols)
    for p in range(pairs):
        picked[p] = jnp.dot(
            onehot[p * per_pair : (p + 1) * per_pair, :], everything, preferred_element_type=F32
        ).astype(BF16)
    mine = x // 2
    piece = per_pair // 2

    def cut(ref, sub):
        return ref.at[pl.ds(sub * piece, piece), :]

    for sub in range(2):
        for k in ORDER:
            to = near(REACH[k])
            c = remote(
                cut(picked.at[to // 2], sub),
                cut(rows.at[h, x], sub),
                direct_send.at[2 * k + sub],
                direct_recv.at[2 * k + sub],
                {"ep_1": to},
            )
            c.start()
            sent.append(c)
        c = remote(
            cut(picked.at[mine], sub),
            cut(rows.at[h, x], sub),
            pair_send.at[sub],
            pair_recv.at[sub],
            {"ep_1": near(1)},
        )
        c.start()
        sent.append(c)
    rows[h, x] = picked[mine]
    crossing = []

    def cross(source, sub, at):
        block = cut(rows.at[h, source], sub)
        c = remote(
            block, block, core_send.at[2 * at + sub], core_recv.at[2 * at + sub], {"hp": other}
        )
        c.start()
        sent.append(c)
        there = cut(rows.at[other, source], sub)
        crossing.append(
            remote(
                there, there, core_send.at[2 * at + sub], core_recv.at[2 * at + sub], {"hp": other}
            )
        )

    cross(x, 0, 0)
    cross(x, 1, 0)
    for sub in range(2):
        for k in (1, 2, 3):
            source = near(-k)
            block = cut(rows.at[h, source], sub)
            at = 2 * k + sub
            remote(
                block, block, direct_send.at[at], direct_recv.at[at], {"ep_1": near(1)}
            ).wait_recv()
            c = remote(block, block, pair_send.at[at], pair_recv.at[at], {"ep_1": near(1)})
            c.start()
            sent.append(c)
            cross(source, sub, k)
    for sub in range(2):
        for k in range(4):
            source = near(1 + k)
            block = cut(rows.at[h, source], sub)
            at = 2 * k + sub
            remote(block, block, pair_send.at[at], pair_recv.at[at], {"ep_1": near(1)}).wait_recv()
            cross(source, sub, 4 + k)
    for c in crossing:
        c.wait_recv()
    for c in sent:
        c.wait_send()


def return_kernel(
    nz,
    nx,
    part,
    info_all,
    stream,
    out,
    from_core,
    for_pair,
    from_pair,
    for_source,
    back,
    mix_high,
    mix_low,
    terms,
    moving,
    landed,
    final,
    core_send,
    core_recv,
    pair_send,
    pair_recv,
    direct_send,
    direct_recv,
    z_send,
    z_recv,
    last_send,
    last_recv,
):
    z, x, h, near = places_around(nz, nx)
    other = 1 - h
    greet(friends(nz, z, h, near))
    tokens, cols = stream.shape
    pairs, per_pair = back.shape[0], back.shape[1]
    mine = pl.multiple_of(h * cols, cols)
    theirs = pl.multiple_of(other * cols, cols)
    sent = []
    arrivals = {}
    order = (4, 3, 2, 1, -3, -2, -1, 0)
    for at, by in enumerate(order):
        source = near(by)
        c = remote(
            part.at[source, :, pl.ds(theirs, cols)],
            from_core.at[source],
            core_send.at[at],
            core_recv.at[at],
            {"hp": other},
        )
        c.start()
        sent.append(c)
        arrivals[by] = c
    slots = pairs * per_pair
    first = (z * slots).astype(F32)
    target = lax.broadcasted_iota(jnp.int32, (slots, 128), 0).astype(F32) + first
    lower = lax.broadcasted_iota(jnp.int32, (8, 128), 1) < tokens
    for j in range(nz // 2):
        both = jnp.where(lower, info_all[2 * j], info_all[2 * j + 1])
        mix = jnp.zeros((slots, 128), F32)
        for k in range(4):
            mix = jnp.where(both[k : k + 1, :] == target, both[4 + k : 5 + k, :], mix)
        high = mix.astype(BF16)
        mix_high[:, 128 * j : 128 * (j + 1)] = high
        mix_low[:, 128 * j : 128 * (j + 1)] = (mix - high.astype(F32)).astype(BF16)

    def whole(by):
        source = near(by)
        arrivals[by].wait_recv()
        return part[source, :, pl.ds(mine, cols)].astype(F32) + from_core[source].astype(F32)

    for k in (3, 2, 1, 0):
        for_pair[k] = whole(1 + k).astype(BF16)
        c = remote(
            for_pair.at[k], from_pair.at[k], pair_send.at[k], pair_recv.at[k], {"ep_1": near(1)}
        )
        c.start()
        sent.append(c)
    pair = x // 2
    for k in (3, 2, 1):
        value = whole(-k)
        remote(
            for_pair.at[k], from_pair.at[k], pair_send.at[k], pair_recv.at[k], {"ep_1": near(1)}
        ).wait_recv()
        for_source[k] = (value + from_pair[k].astype(F32)).astype(BF16)
        c = remote(
            for_source.at[k],
            back.at[pair],
            direct_send.at[k],
            direct_recv.at[k],
            {"ep_1": near(-k)},
        )
        c.start()
        sent.append(c)
    value = whole(0)
    remote(
        for_pair.at[0], from_pair.at[0], pair_send.at[0], pair_recv.at[0], {"ep_1": near(1)}
    ).wait_recv()
    back[pair] = (value + from_pair[0].astype(F32)).astype(BF16)
    for k in ORDER:
        there = back.at[near(REACH[k]) // 2]
        remote(
            there, there, direct_send.at[k], direct_recv.at[k], {"ep_1": near(REACH[k])}
        ).wait_recv()
    results = back[...].reshape(slots, cols)
    over = (((0,), (0,)), ((), ()))
    for j in range(nz // 2):
        at = slice(128 * j, 128 * (j + 1))
        value = lax.dot_general(mix_high[:, at], results, over, preferred_element_type=F32)
        value = value + lax.dot_general(mix_low[:, at], results, over, preferred_element_type=F32)
        terms[2 * j : 2 * j + 2] = value.astype(BF16).reshape(2, tokens, cols)
    half = nz // 2
    subs = 2
    span = tokens // subs
    ways = ((0, shifted(z, 1, nz), half), (1, shifted(z, -1, nz), half - 1))

    def owner(way, step, total):
        return shifted(z, total + 1 - step, nz) if way == 0 else shifted(z, step - total - 1, nz)

    def hop(way, to, step, sub, src):
        at = (way * half + step - 1) * subs + sub
        return remote(
            src,
            landed.at[way, step - 1, pl.ds(sub * span, span), :],
            z_send.at[at],
            z_recv.at[at],
            {"ep_0": to},
        )

    hops = {}
    for step in range(1, half + 1):
        for sub in range(subs):
            at = pl.ds(sub * span, span)
            for way, to, total in ways:
                if step > total:
                    continue
                own = owner(way, step, total)
                if step == 1:
                    c = hop(way, to, step, sub, terms.at[own, at, :])
                else:
                    hops[way, step - 1, sub].wait_recv()
                    moving[way, step - 1, at, :] = (
                        terms[own, at, :].astype(F32) + landed[way, step - 2, at, :].astype(F32)
                    ).astype(BF16)
                    c = hop(way, to, step, sub, moving.at[way, step - 1, at, :])
                c.start()
                sent.append(c)
                hops[way, step, sub] = c
    for sub in range(subs):
        for way, to, total in ways:
            hops[way, total, sub].wait_recv()
    final[...] = (
        stream[...]
        + terms[z].astype(F32)
        + landed[0, half - 1].astype(F32)
        + landed[1, half - 2].astype(F32)
    ).astype(BF16)
    rows = out.shape[0]
    swap = remote(
        final.at[pl.ds(pl.multiple_of(other * rows, rows), rows), :],
        out.at[:, pl.ds(mine, cols)],
        last_send,
        last_recv,
        {"hp": other},
    )
    swap.start()
    out[:, pl.ds(mine, cols)] = final[pl.ds(pl.multiple_of(h * rows, rows), rows), :]
    there = out.at[:, pl.ds(theirs, cols)]
    remote(there, there, last_send, last_recv, {"hp": other}).wait_recv()
    swap.wait_send()
    for c in sent:
        c.wait_send()


def vmem(n):
    return [pl.BlockSpec(memory_space=pltpu.VMEM)] * n


def params(number):
    return pltpu.CompilerParams(collective_id=number, has_side_effects=True)


def picks(blocks, padded, used):
    out = np.zeros((blocks * used, blocks * padded), np.float32)
    for b in range(blocks):
        for i in range(used):
            out[b * used + i, b * padded + i] = 1.0
    return jnp.asarray(out, BF16)


def on_device(
    x_pre,
    x_dec,
    prefill_query_rows,
    prefill_key_values,
    decode_query_rows,
    decode_key_values,
    cache,
    cache_len,
    sinks,
    o_weight,
    norm_gain,
    expert_ids,
    route_logits,
    w_gate_up,
    w_down,
):
    nz, nx = lax.axis_size("ep_0"), lax.axis_size("ep_1")
    dma = pltpu.SemaphoreType.DMA
    width = x_pre.shape[1]
    cols = width // 2
    tokens, topk = expert_ids.shape
    experts = nz * nx // 2
    pairs = nx // 2
    slot = 6
    per_pair = nz * slot
    slots = pairs * per_pair

    earlier = jnp.arange(tokens)[:, None, None, None] < jnp.arange(tokens)[None, None, :, None]
    same = expert_ids[:, :, None, None] == expert_ids[None, None, :, :]
    rank = jnp.sum((earlier & same).astype(jnp.int32), axis=(0, 1))
    z = lax.axis_index("ep_0")
    code = expert_ids // pairs * slots + expert_ids % pairs * per_pair + z * slot + rank
    mix = jax.nn.softmax(route_logits, axis=-1)
    info = jnp.concatenate([code.astype(F32), mix], axis=1).T
    info = jnp.concatenate([info] * (128 // tokens), axis=1)

    attn = attention(
        prefill_query_rows,
        prefill_key_values,
        decode_query_rows,
        decode_key_values,
        cache,
        cache_len,
        sinks,
    )
    attn = jnp.concatenate([attn, jnp.zeros((128 - tokens, attn.shape[1]), BF16)], axis=0)
    heads, per = o_weight.shape
    padded = 16
    weight = jnp.pad(o_weight.T, ((0, padded - per), (0, 0)))
    k_half = heads // 2
    stream, normed, info_all = pl.pallas_call(
        functools.partial(project_kernel, nz, nx, per),
        out_shape=[
            jax.ShapeDtypeStruct((tokens, cols), F32),
            jax.ShapeDtypeStruct((tokens, cols), BF16),
            jax.ShapeDtypeStruct((nz, 8, 128), F32),
        ],
        in_specs=vmem(8),
        out_specs=vmem(3),
        scratch_shapes=[
            pltpu.VMEM((nx, padded, k_half), BF16),
            pltpu.VMEM((nz, padded, k_half), BF16),
            pltpu.VMEM((nz, nx * per, k_half), BF16),
            pltpu.VMEM((nx, nz * per, k_half), BF16),
            pltpu.VMEM((width, 128), F32),
            pltpu.VMEM((width, 128), F32),
            pltpu.VMEM((cols, 128), F32),
            pltpu.VMEM((tokens, 128), F32),
            pltpu.VMEM((tokens, 128), F32),
            ring_sems(nx, 1),
            ring_sems(nx, 1),
            ring_sems(nz, 1),
            ring_sems(nz, 1),
            ring_sems(nz, 2),
            ring_sems(nz, 2),
            ring_sems(nx, 4),
            ring_sems(nx, 4),
            ring_sems(nz, 1),
            ring_sems(nz, 1),
            dma((2,)),
            dma((2,)),
        ],
        compiler_params=params(1),
        name="project",
    )(
        weight,
        attn,
        x_pre,
        x_dec,
        norm_gain.reshape(1, width),
        info,
        picks(nx, padded, per),
        picks(nz, padded, per),
    )
    rows = pl.pallas_call(
        functools.partial(dispatch_kernel, nz, nx),
        out_shape=jax.ShapeDtypeStruct((2, nx, per_pair, cols), BF16),
        in_specs=vmem(2),
        out_specs=vmem(1)[0],
        scratch_shapes=[
            pltpu.VMEM((nz, tokens, cols), BF16),
            pltpu.VMEM((slots, nz * tokens), BF16),
            pltpu.VMEM((pairs, per_pair, cols), BF16),
            ring_sems(nz, 2),
            ring_sems(nz, 2),
            dma((8,)),
            dma((8,)),
            dma((8,)),
            dma((8,)),
            dma((16,)),
            dma((16,)),
        ],
        compiler_params=params(2),
        name="dispatch",
    )(normed, info_all)
    rows = rows.reshape(2, nx * per_pair, cols)

    def into(w):
        return jnp.dot(rows[0], w[:cols], preferred_element_type=F32) + jnp.dot(
            rows[1], w[cols:], preferred_element_type=F32
        )

    gate = into(w_gate_up[0, 0])
    upper = into(w_gate_up[0, 1])
    hidden = ((upper + 1.0) * gate * jax.nn.sigmoid(1.702 * gate)).astype(BF16)
    part = jnp.dot(hidden, w_down[0], preferred_element_type=F32).astype(BF16)
    part = part.reshape(nx, per_pair, width)
    half = nz // 2
    return pl.pallas_call(
        functools.partial(return_kernel, nz, nx),
        out_shape=jax.ShapeDtypeStruct((tokens // 2, width), BF16),
        in_specs=vmem(3),
        out_specs=vmem(1)[0],
        scratch_shapes=[
            pltpu.VMEM((nx, per_pair, cols), BF16),
            pltpu.VMEM((4, per_pair, cols), BF16),
            pltpu.VMEM((4, per_pair, cols), BF16),
            pltpu.VMEM((4, per_pair, cols), BF16),
            pltpu.VMEM((pairs, per_pair, cols), BF16),
            pltpu.VMEM((slots, nz * tokens), BF16),
            pltpu.VMEM((slots, nz * tokens), BF16),
            pltpu.VMEM((nz, tokens, cols), BF16),
            pltpu.VMEM((2, half, tokens, cols), BF16),
            pltpu.VMEM((2, half, tokens, cols), BF16),
            pltpu.VMEM((tokens, cols), BF16),
            dma((8,)),
            dma((8,)),
            dma((4,)),
            dma((4,)),
            dma((4,)),
            dma((4,)),
            ring_sems(nz, 2),
            ring_sems(nz, 2),
            dma,
            dma,
        ],
        compiler_params=params(3),
        name="give_back",
    )(part, info_all, stream)


def solution(mesh):
    torus = Mesh(
        mesh.devices.reshape(mesh.shape["groups"], 16, 8, mesh.shape["hp"]),
        ("groups", "ep_0", "ep_1", "hp"),
    )
    return jax.shard_map(
        on_device,
        mesh=torus,
        in_specs=(
            P(GROUPS_EP, None),
            P(GROUPS_EP, None),
            P(GROUPS_EP, "hp"),
            P(None, GROUPS_EP, "hp"),
            P(GROUPS_EP, "hp"),
            P(None, GROUPS_EP, "hp"),
            P(None, GROUPS_EP, None, "hp"),
            P(GROUPS_EP),
            P("hp"),
            P("hp", EP),
            P(),
            P(GROUPS_EP, None),
            P(GROUPS_EP, None),
            P(EP, None, None, "hp"),
            P(EP, "hp", None),
        ),
        out_specs=P(GROUPS_EP_HP, None),
        check_vma=False,
    )
```

```python
import functools

import jax
import jax.numpy as jnp
import numpy as np
from jax import lax
from jax.experimental import pallas as pl
from jax.experimental.pallas import tpu as pltpu
from jax.sharding import Mesh
from jax.sharding import PartitionSpec as P

HEAD_SIZE = 64
EP = ("ep_0", "ep_1")
GROUPS_EP = ("groups", "ep_0", "ep_1")
GROUPS_EP_HP = ("groups", "ep_0", "ep_1", "hp")
EPS = 1e-05
SLOT = 6
MESH = pl.DeviceIdType.MESH
F32 = jnp.float32
BF16 = jnp.bfloat16


def remote(src, dst, send_sem, recv_sem, where):
    return pltpu.make_async_remote_copy(
        src_ref=src,
        dst_ref=dst,
        send_sem=send_sem,
        recv_sem=recv_sem,
        device_id=where,
        device_id_type=MESH,
    )


def greet(places):
    barrier = pltpu.get_barrier_semaphore()
    for place in places:
        pl.semaphore_signal(barrier, inc=1, device_id=place, device_id_type=MESH)
    pl.semaphore_wait(barrier, len(places))


def shifted(me, by, n):
    return lax.rem(me + (by + 2 * n), n)


def ring_gather(axis, n, me, view, subs, send_sems, recv_sems, sent):
    half = n // 2
    ways = ((0, -1, shifted(me, 1, n)), (1, 1, shifted(me, -1, n)))

    def used(step, way, sub):
        return step < half or sub % 2 == way

    def copy(step, way, sign, to, sub):
        block = view(shifted(me, sign * (step - 1), n), sub)
        at = (way * half + step - 1) * subs + sub
        return remote(block, block, send_sems.at[at], recv_sems.at[at], {axis: to})

    def arrival(step, way, sign, to, sub):
        block = view(shifted(me, sign * step, n), sub)
        at = (way * half + step - 1) * subs + sub
        return remote(block, block, send_sems.at[at], recv_sems.at[at], {axis: to})

    for sub in range(subs):
        for way, sign, to in ways:
            if used(1, way, sub):
                c = copy(1, way, sign, to, sub)
                c.start()
                sent.append(c)
    yield
    for step in range(1, half + 1):
        for sub in range(subs):
            for way, sign, to in ways:
                if not used(step, way, sub):
                    continue
                arrival(step, way, sign, to, sub).wait_recv()
                if step < half and used(step + 1, way, sub):
                    c = copy(step + 1, way, sign, to, sub)
                    c.start()
                    sent.append(c)
        yield


def place_of(way, step, n):
    if step == 0:
        return 0
    if step == n // 2:
        return n - 1
    return 2 * step - 1 + way


def ring_gather_near(axis, n, me, view, subs, send_sems, recv_sems, sent):
    half = n // 2
    ways = ((0, shifted(me, 1, n)), (1, shifted(me, -1, n)))

    def used(step, way, sub):
        return step < half or sub % 2 == way

    def copy(step, way, to, sub):
        at = (way * half + step - 1) * subs + sub
        return remote(
            view(place_of(way, step - 1, n), sub),
            view(place_of(way, step, n), sub),
            send_sems.at[at],
            recv_sems.at[at],
            {axis: to},
        )

    flights = {}

    def launch(step, way, to, sub):
        c = copy(step, way, to, sub)
        c.start()
        sent.append(c)
        flights[step, way, sub] = c

    for sub in range(subs):
        for way, to in ways:
            if used(1, way, sub):
                launch(1, way, to, sub)
    yield
    for step in range(1, half + 1):
        for sub in range(subs):
            for way, to in ways:
                if not used(step, way, sub):
                    continue
                flights[step, way, sub].wait_recv()
                if step < half and used(step + 1, way, sub):
                    launch(step + 1, way, to, sub)
        yield


def ring_sems(n, subs):
    return pltpu.SemaphoreType.DMA((n * subs,))


def nt(a, b):
    return lax.dot_general(a, b, (((1,), (1,)), ((), ())), preferred_element_type=F32)


def iota(shape, dim):
    return lax.broadcasted_iota(jnp.int32, shape, dim)


def probability(scores, sink):
    top = jnp.maximum(jnp.max(scores, axis=-1, keepdims=True), sink)
    expo = jnp.exp(scores - top)
    total = jnp.sum(expo, axis=-1, keepdims=True) + jnp.exp(sink - top)
    return expo, total, top


def attention(pq, pkv, dq, dkv, cache, cache_len, sinks, attn):
    n_pre, n_dec = pq.shape[0], dq.shape[0]
    kv_heads = pkv.shape[2] // HEAD_SIZE
    q_heads = pq.shape[1] // HEAD_SIZE
    group = q_heads // kv_heads
    kv_max = cache.shape[2]
    scale = HEAD_SIZE ** (-0.5)
    visible = iota((n_pre, n_pre), 1) <= iota((n_pre, n_pre), 0)
    attn[n_pre + n_dec :, :] = jnp.zeros((attn.shape[0] - n_pre - n_dec, attn.shape[1]), F32)
    for g in range(q_heads):
        at = slice(g * HEAD_SIZE, (g + 1) * HEAD_SIZE)
        j = g // group
        kv = slice(j * HEAD_SIZE, (j + 1) * HEAD_SIZE)
        scores = nt(pq[:, at], pkv[0, :, kv]) * scale
        scores = jnp.where(visible, scores, -jnp.inf)
        expo, total, _ = probability(scores, sinks[:, g : g + 1])
        weight = (expo / total).astype(BF16)
        value = jnp.dot(weight, pkv[1, :, kv], preferred_element_type=F32)
        attn[0:n_pre, at] = value.astype(BF16).astype(F32)
        if g % 2 == 1:
            yield
    rows = group * n_dec
    which = lax.rem(iota((rows, kv_max), 0), n_dec)
    live = iota((n_dec, kv_max), 1) < cache_len[...]
    live = jnp.concatenate([live.astype(F32)] * group, axis=0) > 0.5
    every = dq[...].astype(F32)
    for j in range(kv_heads):
        kv = slice(j * HEAD_SIZE, (j + 1) * HEAD_SIZE)
        heads = range(j * group, (j + 1) * group)
        queries = jnp.concatenate(
            [every[:, g * HEAD_SIZE : (g + 1) * HEAD_SIZE] for g in heads], axis=0
        )
        narrow = queries.astype(BF16)
        scores = jnp.zeros((rows, kv_max), F32)
        for s in range(n_dec):
            scores = jnp.where(which == s, nt(narrow, cache[0, s, :, kv]), scores)
        scores = jnp.where(live, scores * scale, -jnp.inf)
        own_key = jnp.concatenate([dkv[0, :, kv].astype(F32)] * group, axis=0)
        own_value = jnp.concatenate([dkv[1, :, kv].astype(F32)] * group, axis=0)
        own = jnp.sum(queries * own_key, axis=-1, keepdims=True) * scale
        sink = jnp.concatenate(
            [jnp.broadcast_to(sinks[:, g : g + 1], (n_dec, 1)) for g in heads], axis=0
        )
        top = jnp.maximum(jnp.maximum(jnp.max(scores, axis=-1, keepdims=True), own), sink)
        expo = jnp.exp(scores - top)
        own = jnp.exp(own - top)
        total = jnp.sum(expo, axis=-1, keepdims=True) + own + jnp.exp(sink - top)
        weight = expo / total
        yield
        value = (own / total).astype(BF16).astype(F32) * own_value
        for s in range(n_dec):
            value = value + jnp.dot(
                jnp.where(which == s, weight, 0.0).astype(BF16),
                cache[1, s, :, kv],
                preferred_element_type=F32,
            )
        value = value.astype(BF16).astype(F32)
        for i, g in enumerate(heads):
            attn[n_pre : n_pre + n_dec, g * HEAD_SIZE : (g + 1) * HEAD_SIZE] = value[
                i * n_dec : (i + 1) * n_dec
            ]
        yield


def routes(nz, nx, groups, z, expert_ids, route_logits):
    tokens, topk = expert_ids.shape
    pairs = nx // 2
    near = nz // groups
    ids = expert_ids[...].astype(F32)
    lane = iota((tokens, 128), 1).astype(F32)
    named = jnp.zeros((tokens, 128), F32)
    for k in range(topk):
        named = jnp.where(lane == ids[:, k : k + 1], 1.0, named)
    before = (iota((tokens, tokens), 1) < iota((tokens, tokens), 0)).astype(F32).astype(BF16)
    count = jnp.dot(before, named.astype(BF16), preferred_element_type=F32)
    logits = route_logits[...]
    expo = jnp.exp(logits - jnp.max(logits, axis=-1, keepdims=True))
    mix = expo / jnp.sum(expo, axis=-1, keepdims=True)
    there = jnp.floor(ids * (1.0 / pairs))
    pair = ids - there * pairs
    ahead = z.astype(F32) - there
    ahead = jnp.where(ahead < 0.0, ahead + nz, ahead)
    half = nz // 2
    spot = jnp.where(
        ahead < half, 2.0 * ahead, jnp.where(ahead == half, nz - 1.0, 2.0 * nz - 1.0 - 2.0 * ahead)
    )
    group = jnp.floor(spot * (1.0 / near))
    code = ((there * groups + group) * pairs + pair) * (near * SLOT) + (spot - group * near) * SLOT
    table = jnp.zeros((tokens, 128), F32)
    for k in range(topk):
        rank = jnp.sum(jnp.where(lane == ids[:, k : k + 1], count, 0.0), axis=-1, keepdims=True)
        table = jnp.where(lane == k, code[:, k : k + 1] + rank, table)
        table = jnp.where(lane == 4 + k, mix[:, k : k + 1], table)
    table = jnp.concatenate([table] * (128 // tokens), axis=0)
    return jnp.transpose(table)[0:8]


def project_kernel(
    nz,
    nx,
    groups,
    k_a,
    weight,
    pq,
    pkv,
    dq,
    dkv,
    cache,
    cache_len,
    sinks,
    x_pre,
    x_dec,
    gain,
    expert_ids,
    route_logits,
    pick_a,
    pick_b,
    stream,
    normed,
    info_all,
    attn,
    small_a,
    small_b,
    big_a,
    big_b,
    sum_a,
    sum_b,
    from_core,
    squares,
    squares_in,
    small_a_send,
    small_a_recv,
    small_b_send,
    small_b_recv,
    big_a_send,
    big_a_recv,
    big_b_send,
    big_b_recv,
    info_send,
    info_recv,
    core_send,
    core_recv,
):
    z, x, h = lax.axis_index("ep_0"), lax.axis_index("ep_1"), lax.axis_index("hp")
    other = 1 - h
    greet(
        [
            {"ep_0": shifted(z, 1, nz)},
            {"ep_0": shifted(z, -1, nz)},
            {"ep_1": shifted(x, 1, nx)},
            {"ep_1": shifted(x, -1, nx)},
            {"hp": other},
        ]
    )
    heads, w = weight.shape
    tokens, cols = stream.shape
    padded = small_a.shape[1]
    eye = (iota((padded, w), 0) == iota((padded, w), 1)).astype(F32).astype(BF16)
    turned = nt(eye, weight[...]).astype(BF16)
    small_a[x] = turned[:, 0:k_a]
    small_b[z] = turned[:, k_a:heads]
    sent = []
    ring_a = ring_gather(
        "ep_1", nx, x, lambda b, s: small_a.at[b], 1, small_a_send, small_a_recv, sent
    )
    ring_b = ring_gather(
        "ep_0", nz, z, lambda b, s: small_b.at[b], 1, small_b_send, small_b_recv, sent
    )
    next(ring_a)
    next(ring_b)
    info_all[0] = routes(nz, nx, groups, z, expert_ids, route_logits)
    tell = ring_gather_near(
        "ep_0", nz, z, lambda b, s: info_all.at[b], 1, info_send, info_recv, sent
    )
    next(tell)
    work = attention(pq, pkv, dq, dkv, cache, cache_len, sinks, attn)
    a_rows = big_a.shape[1]
    b_rows = big_b.shape[1]
    for _ in range(nx // 2):
        next(work, None)
        next(ring_a)
        next(ring_b)
    packed = jnp.dot(pick_a[...], small_a[...].reshape(nx * padded, k_a), preferred_element_type=F32)
    big_a[z] = packed.astype(BF16)
    large_a = ring_gather(
        "ep_0",
        nz,
        z,
        lambda b, s: big_a.at[b, pl.ds(s * (a_rows // 2), a_rows // 2), :],
        2,
        big_a_send,
        big_a_recv,
        sent,
    )
    next(large_a)
    for _ in range(nz // 2 - nx // 2):
        next(ring_b)
        next(work, None)
        next(large_a)
        next(tell)
    packed = jnp.dot(
        pick_b[...], small_b[...].reshape(nz * padded, heads - k_a), preferred_element_type=F32
    )
    big_b[x] = packed.astype(BF16)
    large_b = ring_gather(
        "ep_1",
        nx,
        x,
        lambda b, s: big_b.at[b, pl.ds(s * (b_rows // 4), b_rows // 4), :],
        4,
        big_b_send,
        big_b_recv,
        sent,
    )
    next(large_b)
    for _ in range(nx // 2):
        next(large_a)
        next(work, None)
        next(work, None)
        next(tell)
        next(large_b)
    for _ in work:
        pass
    attn_a = attn[:, 0:k_a].astype(BF16)
    attn_b = attn[:, k_a:heads].astype(BF16)
    for b in range(nz):
        sum_a[b * a_rows : (b + 1) * a_rows, :] = nt(big_a[b], attn_a)
    for b in range(nx):
        sum_b[b * b_rows : (b + 1) * b_rows, :] = nt(big_b[b], attn_b)
    for b in range(nz):
        for c in range(nx):
            at_a = (b * nx + c) * w
            at_b = (c * nz + b) * w
            sum_a[at_a : at_a + w, :] = sum_a[at_a : at_a + w, :] + sum_b[at_b : at_b + w, :]
    mine = pl.multiple_of(h * cols, cols)
    theirs = pl.multiple_of(other * cols, cols)
    swap = remote(
        sum_a.at[pl.ds(theirs, cols), :],
        from_core,
        core_send.at[0],
        core_recv.at[0],
        {"hp": other},
    )
    swap.start()
    swap.wait()
    summed = jnp.transpose(sum_a[pl.ds(mine, cols), :] + from_core[...])
    n_pre = x_pre.shape[0]
    stream[0:n_pre, :] = summed[0:n_pre] + x_pre[:, pl.ds(mine, cols)].astype(F32)
    stream[n_pre:tokens, :] = summed[n_pre:tokens] + x_dec[:, pl.ds(mine, cols)].astype(F32)
    value = stream[...]
    total = jnp.sum(value * value, axis=-1, keepdims=True)
    squares[...] = jnp.broadcast_to(total, squares.shape)
    swap = remote(squares, squares_in, core_send.at[1], core_recv.at[1], {"hp": other})
    swap.start()
    swap.wait()
    total = total + squares_in[:, 0:1]
    scale = lax.rsqrt(total / (2 * cols) + EPS)
    normed[...] = (value * scale * gain[:, pl.ds(mine, cols)]).astype(BF16)
    for c in sent:
        c.wait_send()


def places_around(nz, nx):
    z, x, h = lax.axis_index("ep_0"), lax.axis_index("ep_1"), lax.axis_index("hp")
    sign = 1 - 2 * lax.rem(x, 2)

    def near(by):
        return lax.rem(x + by * sign + 2 * nx, nx)

    return z, x, h, near


REACH = {1: -1, 2: 2, 3: -3}
ORDER = (3, 2, 1)


def friends(nz, z, h, near):
    return [
        {"ep_0": shifted(z, 1, nz)},
        {"ep_0": shifted(z, -1, nz)},
        {"hp": 1 - h},
        {"ep_1": near(1)},
        {"ep_1": near(-1)},
        {"ep_1": near(2)},
        {"ep_1": near(-2)},
        {"ep_1": near(-3)},
    ]


def experts_kernel(
    nz,
    nx,
    groups,
    normed,
    info_all,
    stream,
    w_in,
    w_out,
    out,
    gate_up,
    down,
    tok,
    onehot,
    mix_high,
    mix_low,
    picked,
    rows,
    part,
    from_core,
    for_pair,
    from_pair,
    for_source,
    back,
    terms,
    moving,
    landed,
    final,
    load_sem,
    z_send,
    z_recv,
    direct_send,
    direct_recv,
    pair_send,
    pair_recv,
    core_send,
    core_recv,
    sums_send,
    sums_recv,
    up_send,
    up_recv,
    home_send,
    home_recv,
    add_send,
    add_recv,
    last_send,
    last_recv,
):
    z, x, h, near = places_around(nz, nx)
    other = 1 - h
    loads = [
        pltpu.make_async_copy(w_in.at[0], gate_up, load_sem.at[0]),
        pltpu.make_async_copy(w_out.at[0], down, load_sem.at[1]),
    ]
    for c in loads:
        c.start()
    greet(friends(nz, z, h, near))
    tokens, cols = normed.shape
    pairs = nx // 2
    spots = nz // groups
    per = spots * SLOT
    block = pairs * per
    mine = x // 2
    sent = []
    tok[0] = normed[...]
    span = tokens // 2
    ring = ring_gather_near(
        "ep_0", nz, z, lambda b, s: tok.at[b, pl.ds(s * span, span), :], 2, z_send, z_recv, sent
    )
    next(ring)
    lower = iota((8, 128), 1) < tokens
    for g in range(groups):
        first = ((z * groups + g) * block).astype(F32)
        target = iota((block, 128), 0).astype(F32) + first
        for i in range(spots // 2):
            j = g * spots + 2 * i
            both = jnp.where(lower, info_all[j], info_all[j + 1])
            hit = jnp.zeros((block, 128), F32)
            mix = jnp.zeros((block, 128), F32)
            for k in range(4):
                same = both[k : k + 1, :] == target
                hit = jnp.where(same, 1.0, hit)
                mix = jnp.where(same, both[4 + k : 5 + k, :], mix)
            at = slice(128 * i, 128 * (i + 1))
            onehot[g, :, at] = hit.astype(BF16)
            high = mix.astype(BF16)
            mix_high[g, :, at] = high
            mix_low[g, :, at] = (mix - high.astype(F32)).astype(BF16)

    def start(c):
        c.start()
        sent.append(c)
        return c

    crossings = {}

    def cross(g, source, at):
        here, there = rows.at[h, g, source], rows.at[other, g, source]
        sems = core_send.at[8 * g + at], core_recv.at[8 * g + at]
        start(remote(here, here, *sems, {"hp": other}))
        crossings[g, at] = remote(there, there, *sems, {"hp": other})

    def dispatch(g):
        blocks = tok[g * spots : (g + 1) * spots].reshape(spots * tokens, cols)
        chosen = jnp.dot(onehot[g], blocks, preferred_element_type=F32).astype(BF16)
        picked[g] = chosen.reshape(pairs, per, cols)
        for k in ORDER:
            to = near(REACH[k])
            start(
                remote(
                    picked.at[g, to // 2],
                    rows.at[h, g, x],
                    direct_send.at[4 * g + k],
                    direct_recv.at[4 * g + k],
                    {"ep_1": to},
                )
            )
        start(
            remote(
                picked.at[g, mine],
                rows.at[h, g, x],
                pair_send.at[4 * g],
                pair_recv.at[4 * g],
                {"ep_1": near(1)},
            )
        )
        rows[h, g, x] = picked[g, mine]
        cross(g, x, 0)

    def pass_on(g):
        for k in (1, 2, 3):
            source = near(-k)
            at = 4 * g + k
            here = rows.at[h, g, source]
            to = {"ep_1": near(1)}
            remote(here, here, direct_send.at[at], direct_recv.at[at], to).wait_recv()
            start(remote(here, here, pair_send.at[at], pair_recv.at[at], to))
            cross(g, source, k)

    def collect(g):
        for k in range(4):
            source = near(1 + k)
            at = 4 * g + k
            here = rows.at[h, g, source]
            to = {"ep_1": near(1)}
            remote(here, here, pair_send.at[at], pair_recv.at[at], to).wait_recv()
            cross(g, source, 4 + k)

    partials = {}

    def feed(g):
        for at in range(8):
            crossings[g, at].wait_recv()
        left = rows[0, g].reshape(nx * per, cols)
        right = rows[1, g].reshape(nx * per, cols)

        def into(i):
            return jnp.dot(left, gate_up[i, 0:cols, :], preferred_element_type=F32) + jnp.dot(
                right, gate_up[i, cols : 2 * cols, :], preferred_element_type=F32
            )

        gate = into(0)
        upper = into(1)
        hidden = ((upper + 1.0) * gate * jax.nn.sigmoid(1.702 * gate)).astype(BF16)
        for i in range(2):
            value = jnp.dot(hidden, down[:, i * cols : (i + 1) * cols], preferred_element_type=F32)
            part[i, g] = value.astype(BF16).reshape(nx, per, cols)
        partials[g] = start(
            remote(
                part.at[other, g], from_core.at[g], sums_send.at[g], sums_recv.at[g], {"hp": other}
            )
        )

    def whole(g, by):
        source = near(by)
        return part[h, g, source].astype(F32) + from_core[g, source].astype(F32)

    def give(g):
        partials[g].wait_recv()
        for k in (3, 2, 1, 0):
            for_pair[g, k] = whole(g, 1 + k).astype(BF16)
            at = 4 * g + k
            start(
                remote(
                    for_pair.at[g, k],
                    from_pair.at[g, k],
                    up_send.at[at],
                    up_recv.at[at],
                    {"ep_1": near(1)},
                )
            )

    def take(g, k):
        at = 4 * g + k
        remote(
            for_pair.at[g, k],
            from_pair.at[g, k],
            up_send.at[at],
            up_recv.at[at],
            {"ep_1": near(1)},
        ).wait_recv()
        return (whole(g, -k) + from_pair[g, k].astype(F32)).astype(BF16)

    def send_home(g):
        for k in (3, 2, 1):
            for_source[g, k] = take(g, k)
            start(
                remote(
                    for_source.at[g, k],
                    back.at[g, mine],
                    home_send.at[4 * g + k],
                    home_recv.at[4 * g + k],
                    {"ep_1": near(-k)},
                )
            )
        back[g, mine] = take(g, 0)

    over = (((0,), (0,)), ((), ()))

    def combine(g):
        for k in ORDER:
            to = near(REACH[k])
            there = back.at[g, to // 2]
            at = 4 * g + k
            remote(there, there, home_send.at[at], home_recv.at[at], {"ep_1": to}).wait_recv()
        results = back[g].reshape(block, cols)
        value = lax.dot_general(mix_high[g], results, over, preferred_element_type=F32)
        value = value + lax.dot_general(mix_low[g], results, over, preferred_element_type=F32)
        terms[g * spots : (g + 1) * spots] = value.astype(BF16).reshape(spots, tokens, cols)

    half = nz // 2
    ways = ((0, shifted(z, 1, nz)), (1, shifted(z, -1, nz)))
    hops = {}

    def reduce_step(step):
        for sub in range(2):
            at = pl.ds(sub * span, span)
            for way, to in ways:
                if step == 1 and sub != way:
                    continue
                distance = half + 1 - step
                spot = place_of(1 - way, distance, nz)
                if step == 1 or (step == 2 and sub != way):
                    src = terms.at[spot, at, :]
                else:
                    hops[way, step - 1, sub].wait_recv()
                    moving[way, step - 1, at, :] = (
                        terms[spot, at, :].astype(F32) + landed[way, step - 2, at, :].astype(F32)
                    ).astype(BF16)
                    src = moving.at[way, step - 1, at, :]
                n = (way * half + step - 1) * 2 + sub
                hops[way, step, sub] = start(
                    remote(
                        src,
                        landed.at[way, step - 1, at, :],
                        add_send.at[n],
                        add_recv.at[n],
                        {"ep_0": to},
                    )
                )

    def reduce_from(g):
        for step in range(1, half + 1):
            if step not in done and (half + 1 - step) * 2 - 1 >= g * spots:
                done.add(step)
                reduce_step(step)

    done = set()
    pace = spots // 2
    last = groups - 1
    for step in range(1, half + 1):
        next(ring)
        g, phase = divmod(step, pace)
        if phase == 0:
            dispatch(g - 1)
        elif phase == pace // 2 and g >= 2:
            pass_on(g - 2)
    for c in loads:
        c.wait()
    for g in range(max(0, groups - 2), groups - 1):
        pass_on(g)
    for g in range(groups):
        if g == last - 1:
            pass_on(last)
        collect(g)
        if g == last:
            give(last - 1)
        feed(g)
    give(last)
    for g in range(last, -1, -1):
        send_home(g)
        if g >= 2:
            give(g - 2)
        if g < last:
            combine(g + 1)
            reduce_from(g + 1)
    combine(0)
    reduce_from(0)
    for sub in range(2):
        for way, _ in ways:
            hops[way, half, sub].wait_recv()
    final[...] = (
        stream[...]
        + terms[0].astype(F32)
        + landed[0, half - 1].astype(F32)
        + landed[1, half - 1].astype(F32)
    ).astype(BF16)
    count = out.shape[0]
    left = pl.multiple_of(h * cols, cols)
    right = pl.multiple_of(other * cols, cols)
    swap = remote(
        final.at[pl.ds(pl.multiple_of(other * count, count), count), :],
        out.at[:, pl.ds(left, cols)],
        last_send,
        last_recv,
        {"hp": other},
    )
    swap.start()
    out[:, pl.ds(left, cols)] = final[pl.ds(pl.multiple_of(h * count, count), count), :]
    there = out.at[:, pl.ds(right, cols)]
    remote(there, there, last_send, last_recv, {"hp": other}).wait_recv()
    swap.wait_send()
    for c in sent:
        c.wait_send()


def vmem(n):
    return [pl.BlockSpec(memory_space=pltpu.VMEM)] * n


def params(number):
    return pltpu.CompilerParams(collective_id=number, has_side_effects=True)


def picks(blocks, padded, used):
    out = np.zeros((blocks * used, blocks * padded), np.float32)
    for b in range(blocks):
        for i in range(used):
            out[b * used + i, b * padded + i] = 1.0
    return jnp.asarray(out, BF16)


def on_device(
    x_pre,
    x_dec,
    prefill_query_rows,
    prefill_key_values,
    decode_query_rows,
    decode_key_values,
    cache,
    cache_len,
    sinks,
    o_weight,
    norm_gain,
    expert_ids,
    route_logits,
    w_gate_up,
    w_down,
):
    nz, nx = lax.axis_size("ep_0"), lax.axis_size("ep_1")
    dma = pltpu.SemaphoreType.DMA
    width = x_pre.shape[1]
    cols = width // 2
    tokens = expert_ids.shape[0]
    pairs = nx // 2
    groups = 4
    heads, w = o_weight.shape
    padded = 16
    k_a = heads * 5 // 8
    stream, normed, info_all = pl.pallas_call(
        functools.partial(project_kernel, nz, nx, groups, k_a),
        out_shape=[
            jax.ShapeDtypeStruct((tokens, cols), F32),
            jax.ShapeDtypeStruct((tokens, cols), BF16),
            jax.ShapeDtypeStruct((nz, 8, 128), F32),
        ],
        in_specs=vmem(15),
        out_specs=vmem(3),
        scratch_shapes=[
            pltpu.VMEM((128, heads), F32),
            pltpu.VMEM((nx, padded, k_a), BF16),
            pltpu.VMEM((nz, padded, heads - k_a), BF16),
            pltpu.VMEM((nz, nx * w, k_a), BF16),
            pltpu.VMEM((nx, nz * w, heads - k_a), BF16),
            pltpu.VMEM((width, 128), F32),
            pltpu.VMEM((width, 128), F32),
            pltpu.VMEM((cols, 128), F32),
            pltpu.VMEM((tokens, 128), F32),
            pltpu.VMEM((tokens, 128), F32),
            ring_sems(nx, 1),
            ring_sems(nx, 1),
            ring_sems(nz, 1),
            ring_sems(nz, 1),
            ring_sems(nz, 2),
            ring_sems(nz, 2),
            ring_sems(nx, 4),
            ring_sems(nx, 4),
            ring_sems(nz, 1),
            ring_sems(nz, 1),
            dma((2,)),
            dma((2,)),
        ],
        compiler_params=params(1),
        name="project",
    )(
        o_weight,
        prefill_query_rows,
        prefill_key_values,
        decode_query_rows,
        decode_key_values,
        cache,
        cache_len.reshape(-1, 1),
        sinks.reshape(1, -1),
        x_pre,
        x_dec,
        norm_gain.reshape(1, width),
        expert_ids,
        route_logits,
        picks(nx, padded, w),
        picks(nz, padded, w),
    )
    half = nz // 2
    spots = nz // groups
    per = spots * SLOT
    block = pairs * per
    anywhere = pl.BlockSpec(memory_space=pl.ANY)
    return pl.pallas_call(
        functools.partial(experts_kernel, nz, nx, groups),
        out_shape=jax.ShapeDtypeStruct((tokens // 2, width), BF16),
        in_specs=vmem(3) + [anywhere, anywhere],
        out_specs=vmem(1)[0],
        scratch_shapes=[
            pltpu.VMEM(w_gate_up.shape[1:], BF16),
            pltpu.VMEM(w_down.shape[1:], BF16),
            pltpu.VMEM((nz, tokens, cols), BF16),
            pltpu.VMEM((groups, block, spots * tokens), BF16),
            pltpu.VMEM((groups, block, spots * tokens), BF16),
            pltpu.VMEM((groups, block, spots * tokens), BF16),
            pltpu.VMEM((groups, pairs, per, cols), BF16),
            pltpu.VMEM((2, groups, nx, per, cols), BF16),
            pltpu.VMEM((2, groups, nx, per, cols), BF16),
            pltpu.VMEM((groups, nx, per, cols), BF16),
            pltpu.VMEM((groups, 4, per, cols), BF16),
            pltpu.VMEM((groups, 4, per, cols), BF16),
            pltpu.VMEM((groups, 4, per, cols), BF16),
            pltpu.VMEM((groups, pairs, per, cols), BF16),
            pltpu.VMEM((nz, tokens, cols), BF16),
            pltpu.VMEM((2, half, tokens, cols), BF16),
            pltpu.VMEM((2, half, tokens, cols), BF16),
            pltpu.VMEM((tokens, cols), BF16),
            dma((2,)),
            ring_sems(nz, 2),
            ring_sems(nz, 2),
            dma((groups * 4,)),
            dma((groups * 4,)),
            dma((groups * 4,)),
            dma((groups * 4,)),
            dma((groups * 8,)),
            dma((groups * 8,)),
            dma((groups,)),
            dma((groups,)),
            dma((groups * 4,)),
            dma((groups * 4,)),
            dma((groups * 4,)),
            dma((groups * 4,)),
            ring_sems(nz, 2),
            ring_sems(nz, 2),
            dma,
            dma,
        ],
        compiler_params=params(2),
        name="layer",
    )(normed, info_all, stream, w_gate_up, w_down)


def solution(mesh):
    torus = Mesh(
        mesh.devices.reshape(mesh.shape["groups"], 16, 8, mesh.shape["hp"]),
        ("groups", "ep_0", "ep_1", "hp"),
    )
    return jax.shard_map(
        on_device,
        mesh=torus,
        in_specs=(
            P(GROUPS_EP, None),
            P(GROUPS_EP, None),
            P(GROUPS_EP, "hp"),
            P(None, GROUPS_EP, "hp"),
            P(GROUPS_EP, "hp"),
            P(None, GROUPS_EP, "hp"),
            P(None, GROUPS_EP, None, "hp"),
            P(GROUPS_EP),
            P("hp"),
            P("hp", EP),
            P(),
            P(GROUPS_EP, None),
            P(GROUPS_EP, None),
            P(EP, None, None, "hp"),
            P(EP, "hp", None),
        ),
        out_specs=P(GROUPS_EP_HP, None),
        check_vma=False,
    )
```
